32 devices in a mesh: trial: 4 (over y, x), rows: 2 (over core), cols: 4 (over z).
Axes of the slice: x: 2, y: 2, z: 4, core: 2. Of those that a mesh axis runs over, the one named last changes fastest.
Arguments:
- weight_gate: float32 [8192, 8192], P(('trial', 'rows'), 'cols'), parts along dimension 0, may hold values from -0.1875 to 0.1875
- moment_gate: float32 [8192, 8192], P(('trial', 'rows'), 'cols'), parts along dimension 0, may hold values from -6 to 6
- square_gate: float32 [8192, 8192], P(('trial', 'rows'), 'cols'), parts along dimension 0, may hold values from 0.1 to 10
- weight_up: float32 [8192, 8192], P(('trial', 'rows'), 'cols'), parts along dimension 0, may hold values from -0.1875 to 0.1875
- moment_up: float32 [8192, 8192], P(('trial', 'rows'), 'cols'), parts along dimension 0, may hold values from -6 to 6
- square_up: float32 [8192, 8192], P(('trial', 'rows'), 'cols'), parts along dimension 0, may hold values from 0.1 to 10
- norm_gain: float32 [8192], P(('trial', 'rows')), parts along dimension 0, may hold values from 0.25 to 1.75
Outputs:
- serving_gate: bfloat16 [8192, 8192], P('trial', 'cols'), parts along dimension 0
- serving_up: bfloat16 [8192, 8192], P('trial', 'cols'), parts along dimension 0
- column_gate: float32 [32768], P(('trial', 'cols')), parts along dimension 0
- column_up: float32 [32768], P(('trial', 'cols')), parts along dimension 0
The draws below stay inside these ranges and needn't reach their ends.
There are 4 independent parts, one for each index of `trial`. The reference program is written for one: setup_inputs(seed, part) draws one part's arguments, and reference() takes and returns one part's arrays. A program takes and returns all parts, laid end to end along the dimension named above; each array names one. Nothing has to cross between parts.
All inputs are finite; a program needn't handle non-finite values. Where the reference program divides by a largest or mean magnitude, that divisor is 1e-20 or more.
Results may differ from the reference program's by a relative error of at most 0.001.
Values may be sent and summed in bfloat16 or wider, within the bound.
A program may use at most 128 MiB of HBM per device.

```python
import math
import jax
import jax.numpy as jnp
from jax import lax

D_MODEL = 2048
D_INNER = 8192


def strengthened(array, stream_key, source, target, blocks, factor):
    def block_of(dim):
        return (jnp.arange(array.shape[dim]) // (array.shape[dim] // blocks)).reshape((-1,) + (1,) * (array.ndim - 1 - dim))

    first = jax.random.permutation(stream_key, blocks)[block_of(target)]
    far = (block_of(target) + blocks // 2) % blocks
    return jnp.where((block_of(source) == first) | (block_of(source) == far), factor * array, array)


def shard_levels(stream_key, extent, cuts, least, high):
    def one(axis_at, shards_of):
        draws = jax.random.uniform(jax.random.fold_in(jax.random.fold_in(stream_key, 6), axis_at), (shards_of,), jnp.float32, least / len(cuts), high / len(cuts))
        return jnp.repeat(jnp.exp(draws), extent[axis_at] // shards_of).reshape((-1,) + (1,) * (len(extent) - axis_at - 1))

    level = one(*cuts[0])
    for cut in cuts[1:]:
        level = level * one(*cut)
    return level


def gaussian(own_key, extent, width, bound, split=(), held_as=jnp.bfloat16):
    drawn = jax.random.normal(own_key, extent, jnp.float32) * width
    if len(split) > 0:
        drawn = shard_levels(own_key, extent, split, -0.22, 0.18) * drawn
    return jnp.clip(drawn, min=-bound, max=bound).astype(held_as)


def bell_draw_with(key, extent, width, bound, shards, heavy, kind=jnp.bfloat16):
    values = width * jax.random.normal(key, extent, jnp.float32)
    if shards:
        values = values * shard_levels(key, extent, shards, -0.22, 0.18)
    return jnp.clip(strengthened(values, jax.random.fold_in(key, 3), *heavy), -bound, bound).astype(kind)


def setup_inputs(seed: int = 0, part: int = 0) -> dict:
    splits = jax.random.split(jax.random.key(seed), 8)
    own_keys = jax.random.split(jax.random.fold_in(splits[7], part), 8)
    return {
        "weight_gate": bell_draw_with(own_keys[0], (D_MODEL, D_INNER), D_MODEL ** -0.5, 0.1875, ((0, 2), (1, 4)), (0, 1, 4, 2.0), jnp.float32),
        "moment_gate": gaussian(own_keys[1], (D_MODEL, D_INNER), 1.0, 6.0, ((0, 2), (1, 4)), jnp.float32),
        "square_gate": jnp.clip(jnp.exp(math.log(10.0) - 4.6051702 * jax.random.uniform(own_keys[2], (D_MODEL, D_INNER), jnp.float32) ** shard_levels(own_keys[2], (D_MODEL, D_INNER), ((0, 2), (1, 4)), -0.2, 0.2)), 0.1, 10.0),
        "weight_up": bell_draw_with(own_keys[3], (D_MODEL, D_INNER), D_MODEL ** -0.5, 0.1875, ((0, 2), (1, 4)), (0, 1, 4, 2.0), jnp.float32),
        "moment_up": gaussian(own_keys[4], (D_MODEL, D_INNER), 1.0, 6.0, ((0, 2), (1, 4)), jnp.float32),
        "square_up": jnp.clip(jnp.exp(math.log(10.0) - 4.6051702 * jax.random.uniform(own_keys[5], (D_MODEL, D_INNER), jnp.float32) ** shard_levels(own_keys[5], (D_MODEL, D_INNER), ((0, 2), (1, 4)), -0.2, 0.2)), 0.1, 10.0),
        "norm_gain": jnp.clip(1.0 + 0.15 * jax.random.normal(own_keys[6], (D_MODEL,), jnp.float32), 0.25, 1.75),
    }


learn_rate = 0.02
decay_rate = 0.05
tiny_value = 1e-08

def reference(weight_gate, moment_gate, square_gate, weight_up, moment_up, square_up, norm_gain):
    whole_gate = weight_gate - learn_rate * (moment_gate / (jnp.sqrt(square_gate) + tiny_value) + decay_rate * weight_gate)
    whole_up = weight_up - learn_rate * (moment_up / (jnp.sqrt(square_up) + tiny_value) + decay_rate * weight_up)
    whole_gained_gate = whole_gate * norm_gain[:, None]
    whole_gained_up = whole_up * norm_gain[:, None]
    column_gate = lax.optimization_barrier(jnp.sum(jnp.abs(whole_gained_gate), axis=0)) / D_MODEL
    serving_gate = (whole_gained_gate / column_gate).astype(jnp.bfloat16)
    column_up = lax.optimization_barrier(jnp.sum(jnp.abs(whole_gained_up), axis=0)) / D_MODEL
    serving_up = (whole_gained_up / column_up).astype(jnp.bfloat16)
    return (serving_gate, serving_up, column_gate, column_up)
```

```python
import functools

import jax
import jax.numpy as jnp
from jax import lax
from jax.experimental import pallas as pl
from jax.experimental.pallas import tpu as pltpu
from jax.sharding import PartitionSpec as P

learn_rate = 0.02
decay_rate = 0.05
tiny_value = 1e-08

LANES = 128
SLAB = 256
SLOTS = 8
REST = 3
MESH = pl.DeviceIdType.MESH


def unit_of(t):
    return t // 2, t % 2


def exchange_kernel(
    n, wg, mg, sg, wu, mu, su, gain_hbm, out_g, out_u, col_g, col_u, rest,
    w_buf, m_buf, s_buf, held, gain, keep_scale, step_scale, parts,
    in_sem, part_send, part_recv, row_send, row_recv, gain_sem,
):
    rows, width = wg.shape
    units = 2 * (width // SLAB)
    bulk = units - REST
    chunk = min(rows, 256)
    me = lax.axis_index("rows")
    sources = ((wg, mg, sg), (wu, mu, su))
    outs = (out_g, out_u)
    cols = (col_g, col_u)
    buffers = (w_buf, m_buf, s_buf)

    def columns(j):
        return pl.ds(pl.multiple_of(j * SLAB, SLAB), SLAB)

    def loads(j, p):
        slot = lax.rem(2 * j + p, SLOTS)
        return [
            pltpu.make_async_copy(source.at[:, columns(j)], buffer.at[slot], in_sem.at[slot, i])
            for i, (source, buffer) in enumerate(zip(sources[p], buffers))
        ]

    def part_copy(j, p, k, owner):
        t = 2 * j + p
        return pltpu.make_async_remote_copy(
            src_ref=parts.at[t, owner],
            dst_ref=parts.at[t, owner],
            send_sem=part_send.at[t, k - 1],
            recv_sem=part_recv.at[t, k - 1],
            device_id={"rows": lax.rem(me + k, n)},
            device_id_type=MESH,
        )

    def row_copy(j, p, k, owner):
        t = 2 * j + p
        block = outs[p].at[pl.ds(pl.multiple_of(owner * rows, rows), rows), columns(j)]
        return pltpu.make_async_remote_copy(
            src_ref=block,
            dst_ref=block,
            send_sem=row_send.at[t, k - 1],
            recv_sem=row_recv.at[t, k - 1],
            device_id={"rows": lax.rem(me + k, n)},
            device_id_type=MESH,
        )

    zero = jnp.zeros((8, LANES), jnp.float32)

    def update(j, p, keep_value):
        slot = lax.rem(2 * j + p, SLOTS)
        for copy in loads(j, p):
            copy.wait()

        def body(c, sums):
            at = pl.ds(pl.multiple_of(c * chunk, chunk), chunk)
            keep, scale = keep_scale[at, :], step_scale[at, :]
            new = []
            for i in range(SLAB // LANES):
                tile = pl.ds(i * LANES, LANES)
                square = s_buf[slot, at, tile]
                root = square * lax.rsqrt(square)
                value = w_buf[slot, at, tile] * keep - (m_buf[slot, at, tile] * scale) / (root + tiny_value)
                keep_value(at, tile, value)
                new.append(sums[i] + jnp.sum(jnp.abs(value).reshape(chunk // 8, 8, LANES), axis=0))
            return tuple(new)

        return lax.fori_loop(0, rows // chunk, body, (zero,) * (SLAB // LANES))

    def update_bulk(j, p):
        def keep_value(at, tile, value):
            held[p, at, tile] = value

        sums = update(j, p, keep_value)
        for i in range(SLAB // LANES):
            parts[2 * j + p, me, :, pl.ds(i * LANES, LANES)] = sums[i]
        for k in range(1, n):
            part_copy(j, p, k, me).start()

    def update_rest(j, p, u):
        def keep_value(at, tile, value):
            rest[u, at, tile] = value

        sums = update(j, p, keep_value)
        for i in range(SLAB // LANES):
            rest[u, pl.ds(rows, 8), pl.ds(i * LANES, LANES)] = sums[i]

    def finish(j, p):
        t = 2 * j + p
        for k in range(1, n):
            part_copy(j, p, k, lax.rem(me + n - k, n)).wait_recv()
        total = parts[t, 0]
        for r in range(1, n):
            total = total + parts[t, r]
        column = jnp.sum(total, axis=0, keepdims=True) / (n * rows)
        cols[p][:, columns(j)] = column
        factor = 1.0 / column

        def body(c, carry):
            at = pl.ds(pl.multiple_of(c * chunk, chunk), chunk)
            to = pl.ds(pl.multiple_of(me * rows + c * chunk, chunk), chunk)
            outs[p][to, columns(j)] = (held[p, at, :] * factor).astype(jnp.bfloat16)
            return carry

        lax.fori_loop(0, rows // chunk, body, 0)
        for k in range(1, n):
            row_copy(j, p, k, me).start()

    gain_copy = pltpu.make_async_copy(gain_hbm, gain, gain_sem)
    gain_copy.start()
    ahead = min(SLOTS, units)

    def begin(j, carry):
        for p in range(2):
            for copy in loads(j, p):
                copy.start()
        return carry

    lax.fori_loop(0, ahead // 2, begin, 0)

    barrier = pltpu.get_barrier_semaphore()
    for k in range(1, n):
        pl.semaphore_signal(barrier, inc=1, device_id={"rows": lax.rem(me + k, n)}, device_id_type=MESH)

    gain_copy.wait()
    for r in range(rows // LANES):
        spread = jnp.broadcast_to(gain[r : r + 1, :], (LANES, LANES)).T
        at = pl.ds(r * LANES, LANES)
        keep_scale[at, :] = spread * (1.0 - learn_rate * decay_rate)
        step_scale[at, :] = spread * learn_rate

    pl.semaphore_wait(barrier, n - 1)

    def refill(j, p):
        @pl.when(2 * j + p + ahead < units)
        def _():
            for copy in loads(j + ahead // 2, p):
                copy.start()

    def step(j, carry):
        update_bulk(j, 0)
        refill(j, 0)

        @pl.when(j > 0)
        def _():
            finish(j - 1, 1)

        update_bulk(j, 1)
        refill(j, 1)
        finish(j, 0)
        return carry

    lax.fori_loop(0, bulk // 2, step, 0)
    waiting = [bulk // 2 * 2 - 1]
    if bulk % 2:
        update_bulk(*unit_of(bulk - 1))
        finish(*unit_of(waiting.pop()))
        waiting.append(bulk - 1)
    for t in range(bulk, units):
        update_rest(*unit_of(t), t - bulk)
        if waiting:
            finish(*unit_of(waiting.pop()))

    def drained(j, p):
        for k in range(1, n):
            part_copy(j, p, k, me).wait_send()
            row_copy(j, p, k, me).wait_send()
            row_copy(j, p, k, lax.rem(me + n - k, n)).wait_recv()

    def drain(j, carry):
        for p in range(2):
            drained(j, p)
        return carry

    lax.fori_loop(0, bulk // 2, drain, 0)
    if bulk % 2:
        drained(*unit_of(bulk - 1))


def store_kernel(pieces, ends, gate, up, out_g, out_u, sem):
    height = gate.shape[0] // pieces
    copies = []
    for p, (source, target) in enumerate(((gate, out_g), (up, out_u))):
        for i in range(pieces):
            at = (pl.ds(i * height, height), pl.ds(0, ends[p]))
            copies.append(pltpu.make_async_copy(source.at[at], target.at[at], sem.at[p, i]))
    for copy in copies:
        copy.start()
    for copy in copies:
        copy.wait()


def rest_kernel(n, bulk, *refs):
    own, peers = refs[0], refs[1:n]
    col_g, col_u, _, _, out_g, out_u, out_cg, out_cu, block, column, sem, col_sem = refs[n:]
    rows = own.shape[1] - 8
    chunk = min(rows, 256)
    me = lax.axis_index("rows")
    outs = (out_g, out_u)
    copies = []
    for u in range(REST):
        j, p = unit_of(bulk + u)
        at_columns = pl.ds(j * SLAB, SLAB)
        tail = pl.ds(rows, 8)
        total = own[u, tail, :]
        for peer in peers:
            total = total + peer[u, tail, :]
        mean = jnp.sum(total, axis=0, keepdims=True) / (n * rows)
        (col_g, col_u)[p][:, at_columns] = mean
        factor = 1.0 / mean
        for k, source in enumerate((own, *peers)):
            owner = lax.rem(me + n - k, n)

            def body(c, carry):
                at = pl.ds(pl.multiple_of(c * chunk, chunk), chunk)
                to = pl.ds(pl.multiple_of(owner * rows + c * chunk, chunk), chunk)
                block[u, to, :] = (source[u, at, :] * factor).astype(jnp.bfloat16)
                return carry

            lax.fori_loop(0, rows // chunk, body, 0)
            to = pl.ds(pl.multiple_of(owner * rows, rows), rows)
            copies.append(pltpu.make_async_copy(block.at[u, to], outs[p].at[to, at_columns], sem.at[u, k]))
            copies[-1].start()
    for p in range(2):
        copies.append(pltpu.make_async_copy((col_g, col_u)[p], (out_cg, out_cu)[p], col_sem.at[p]))
        copies[-1].start()
    for copy in copies:
        copy.wait()


def solution(mesh):
    n = mesh.shape["rows"]

    def shards(weight_gate, moment_gate, square_gate, weight_up, moment_up, square_up, norm_gain):
        rows, width = weight_gate.shape
        units = 2 * (width // SLAB)
        bulk = units - REST
        peers = max(n - 1, 1)
        any_space = pl.BlockSpec(memory_space=pl.ANY)
        in_vmem = pl.BlockSpec(memory_space=pltpu.VMEM)
        full = ((n * rows, width), jnp.bfloat16)
        column = ((1, width), jnp.float32)
        dma = pltpu.SemaphoreType.DMA
        gate, up, col_g, col_u, rest = pl.pallas_call(
            functools.partial(exchange_kernel, n),
            out_shape=tuple(
                pltpu.VMEM(*shape) for shape in (full, full, column, column, ((REST, rows + 8, SLAB), jnp.float32))
            ),
            in_specs=[any_space] * 6 + [pl.BlockSpec(memory_space=pltpu.HBM)],
            out_specs=[in_vmem] * 5,
            scratch_shapes=[
                pltpu.VMEM((SLOTS, rows, SLAB), jnp.float32),
                pltpu.VMEM((SLOTS, rows, SLAB), jnp.float32),
                pltpu.VMEM((SLOTS, rows, SLAB), jnp.float32),
                pltpu.VMEM((2, rows, SLAB), jnp.float32),
                pltpu.VMEM((rows // LANES, LANES), jnp.float32),
                pltpu.VMEM((rows, LANES), jnp.float32),
                pltpu.VMEM((rows, LANES), jnp.float32),
                pltpu.VMEM((bulk, n, 8, SLAB), jnp.float32),
                dma((SLOTS, 3)),
                dma((bulk, peers)),
                dma((bulk, peers)),
                dma((bulk, peers)),
                dma((bulk, peers)),
                dma,
            ],
            compiler_params=pltpu.CompilerParams(
                collective_id=0, has_side_effects=True, vmem_limit_bytes=36 * 1024 * 1024
            ),
            name="exchange",
        )(
            weight_gate, moment_gate, square_gate, weight_up, moment_up, square_up,
            norm_gain.reshape(rows // LANES, LANES),
        )
        others = [
            lax.ppermute(rest, "rows", [(i, (i + k) % n) for i in range(n)]) for k in range(1, n)
        ]
        pieces = 4
        ends = ((bulk + 1) // 2 * SLAB, bulk // 2 * SLAB)
        out_g, out_u = pl.pallas_call(
            functools.partial(store_kernel, pieces, ends),
            out_shape=(jax.ShapeDtypeStruct(*full),) * 2,
            in_specs=[in_vmem] * 2,
            out_specs=[any_space] * 2,
            scratch_shapes=[dma((2, pieces))],
            compiler_params=pltpu.CompilerParams(vmem_limit_bytes=1024 * 1024),
            cost_estimate=pl.CostEstimate(flops=200_000_000, bytes_accessed=4 * n * rows * width, transcendentals=0),
            name="store",
        )(gate, up)
        first = n + 2
        out_g, out_u, out_cg, out_cu = pl.pallas_call(
            functools.partial(rest_kernel, n, bulk),
            out_shape=(jax.ShapeDtypeStruct(*full),) * 2 + (jax.ShapeDtypeStruct(*column),) * 2,
            in_specs=[in_vmem] * first + [any_space] * 2,
            out_specs=[any_space] * 4,
            input_output_aliases={first: 0, first + 1: 1},
            scratch_shapes=[
                pltpu.VMEM((REST, n * rows, SLAB), jnp.bfloat16),
                pltpu.VMEM((1, SLAB), jnp.float32),
                dma((REST, n)),
                dma((2,)),
            ],
            compiler_params=pltpu.CompilerParams(vmem_limit_bytes=8 * 1024 * 1024),
            name="rest",
        )(rest, *others, col_g, col_u, out_g, out_u)
        return out_g, out_u, out_cg.reshape(width), out_cu.reshape(width)

    held = P(("trial", "rows"), "cols")
    return jax.shard_map(
        shards,
        mesh=mesh,
        in_specs=(held,) * 6 + (P(("trial", "rows")),),
        out_specs=(P("trial", "cols"), P("trial", "cols"), P(("trial", "cols")), P(("trial", "cols"))),
        check_vma=False,
    )
```

```python
import functools

import jax
import jax.numpy as jnp
from jax import lax
from jax.experimental import pallas as pl
from jax.experimental.pallas import tpu as pltpu
from jax.sharding import PartitionSpec as P

learn_rate = 0.02
decay_rate = 0.05
tiny_value = 1e-08

LANES = 128
SLAB = 256
SLOTS = 4
RING = 4
READY = 1
REST = 2
MESH = pl.DeviceIdType.MESH


def unit_of(t):
    return t // 2, t % 2


def exchange_kernel(
    n, wg, mg, sg, wu, mu, su, gain_hbm, out_g, out_u, col_g, col_u, ready, rest,
    buf, held, gain, keep_scale, step_scale, parts,
    in_sem, part_send, part_recv, row_send, row_recv, gain_sem, piece_sem,
):
    rows, width = wg.shape
    units = 2 * (width // SLAB)
    whole = units - REST
    bulk = whole - READY
    chunk = min(rows, 256)
    me = lax.axis_index("rows")
    sources = ((wg, mg, sg), (wu, mu, su))
    outs = (out_g, out_u)
    cols = (col_g, col_u)

    def columns(j):
        return pl.ds(pl.multiple_of(j * SLAB, SLAB), SLAB)

    def loads(j, p):
        slot = lax.rem(2 * j + p, SLOTS)
        return [
            pltpu.make_async_copy(source.at[:, columns(j)], buf.at[slot, i], in_sem.at[slot])
            for i, source in enumerate(sources[p])
        ]

    def loaded(slot):
        pltpu.make_async_copy(buf.at[slot], buf.at[slot], in_sem.at[slot]).wait()

    def piece_loads(c):
        j, p = unit_of(units - 1)
        at = pl.ds(pl.multiple_of(c * chunk, chunk), chunk)
        return [
            pltpu.make_async_copy(source.at[at, columns(j)], buf.at[(units - 1) % SLOTS, i, at], piece_sem.at[c])
            for i, source in enumerate(sources[p])
        ]

    def piece_loaded(c):
        block = buf.at[(units - 1) % SLOTS, :, pl.ds(pl.multiple_of(c * chunk, chunk), chunk)]
        pltpu.make_async_copy(block, block, piece_sem.at[c]).wait()

    def part_copy(j, p, k, owner):
        t = 2 * j + p
        return pltpu.make_async_remote_copy(
            src_ref=parts.at[t, owner],
            dst_ref=parts.at[t, owner],
            send_sem=part_send.at[lax.rem(t, RING), k - 1],
            recv_sem=part_recv.at[lax.rem(t, RING), k - 1],
            device_id={"rows": lax.rem(me + k, n)},
            device_id_type=MESH,
        )

    def row_copy(p, k, owner, at_columns):
        block = outs[p].at[pl.ds(pl.multiple_of(owner * rows, rows), rows), at_columns]
        return pltpu.make_async_remote_copy(
            src_ref=block,
            dst_ref=block,
            send_sem=row_send.at[p, k - 1],
            recv_sem=row_recv.at[p, k - 1],
            device_id={"rows": lax.rem(me + k, n)},
            device_id_type=MESH,
        )

    zero = jnp.zeros((8, LANES), jnp.float32)

    def update(j, p, keep_value, pieces=False):
        slot = lax.rem(2 * j + p, SLOTS)
        if not pieces:
            loaded(slot)

        def body(c, sums):
            if pieces:
                piece_loaded(c)
            at = pl.ds(pl.multiple_of(c * chunk, chunk), chunk)
            keep, scale = keep_scale[at, :], step_scale[at, :]
            new = []
            for i in range(SLAB // LANES):
                tile = pl.ds(i * LANES, LANES)
                square = buf[slot, 2, at, tile]
                root = square * lax.rsqrt(square)
                value = buf[slot, 0, at, tile] * keep - (buf[slot, 1, at, tile] * scale) / (root + tiny_value)
                keep_value(at, tile, value)
                new.append(sums[i] + jnp.sum(jnp.abs(value).reshape(chunk // 8, 8, LANES), axis=0))
            return tuple(new)

        return lax.fori_loop(0, rows // chunk, body, (zero,) * (SLAB // LANES))

    def update_shared(j, p):
        def keep_value(at, tile, value):
            held[p, at, tile] = value

        sums = update(j, p, keep_value)
        for i in range(SLAB // LANES):
            parts[2 * j + p, me, :, pl.ds(i * LANES, LANES)] = sums[i]
        for k in range(1, n):
            part_copy(j, p, k, me).start()

    def update_rest(j, p, u):
        def keep_value(at, tile, value):
            rest[u, at, tile] = value

        sums = update(j, p, keep_value, pieces=2 * j + p == units - 1)
        for i in range(SLAB // LANES):
            rest[u, pl.ds(rows, 8), pl.ds(i * LANES, LANES)] = sums[i]

    def factor_of(j, p):
        t = 2 * j + p
        for k in range(1, n):
            part_copy(j, p, k, lax.rem(me + n - k, n)).wait_recv()
            part_copy(j, p, k, me).wait_send()
        total = parts[t, 0]
        for r in range(1, n):
            total = total + parts[t, r]
        column = jnp.sum(total, axis=0, keepdims=True) / (n * rows)
        cols[p][:, columns(j)] = column
        return 1.0 / column

    def finish_ready(j, p):
        factor = factor_of(j, p)

        def body(c, carry):
            at = pl.ds(pl.multiple_of(c * chunk, chunk), chunk)
            ready[2 * j + p - bulk, at, :] = (held[p, at, :] * factor).astype(jnp.bfloat16)
            return carry

        lax.fori_loop(0, rows // chunk, body, 0)

    def finish(j, p):
        factor = factor_of(j, p)

        def body(c, carry):
            at = pl.ds(pl.multiple_of(c * chunk, chunk), chunk)
            to = pl.ds(pl.multiple_of(me * rows + c * chunk, chunk), chunk)
            outs[p][to, columns(j)] = (held[p, at, :] * factor).astype(jnp.bfloat16)
            return carry

        lax.fori_loop(0, rows // chunk, body, 0)
        for k in range(1, n):
            row_copy(p, k, me, columns(j)).start()

    gain_copy = pltpu.make_async_copy(gain_hbm, gain, gain_sem)
    gain_copy.start()
    ahead = min(SLOTS, units)

    def begin(j, carry):
        for p in range(2):
            for copy in loads(j, p):
                copy.start()
        return carry

    lax.fori_loop(0, ahead // 2, begin, 0)

    barrier = pltpu.get_barrier_semaphore()
    for k in range(1, n):
        pl.semaphore_signal(barrier, inc=1, device_id={"rows": lax.rem(me + k, n)}, device_id_type=MESH)

    gain_copy.wait()
    for r in range(rows // LANES):
        spread = jnp.broadcast_to(gain[r : r + 1, :], (LANES, LANES)).T
        at = pl.ds(r * LANES, LANES)
        keep_scale[at, :] = spread * (1.0 - learn_rate * decay_rate)
        step_scale[at, :] = spread * learn_rate

    pl.semaphore_wait(barrier, n - 1)

    def refill(j, p):
        @pl.when(2 * j + p + ahead < units - 1)
        def _():
            for copy in loads(j + ahead // 2, p):
                copy.start()

        if p == (units - 1) % 2:

            @pl.when(2 * j + p + ahead == units - 1)
            def _():
                for c in range(rows // chunk):
                    for copy in piece_loads(c):
                        copy.start()

    def step(j, carry):
        update_shared(j, 0)
        refill(j, 0)

        @pl.when(j > 0)
        def _():
            finish(j - 1, 1)

        update_shared(j, 1)
        refill(j, 1)
        finish(j, 0)
        return carry

    lax.fori_loop(0, bulk // 2, step, 0)
    waiting = [bulk // 2 * 2 - 1]

    def finish_next():
        t = waiting.pop(0)
        (finish if t < bulk else finish_ready)(*unit_of(t))

    for t in range(bulk // 2 * 2, units):
        if t < whole:
            update_shared(*unit_of(t))
            waiting.append(t)
        else:
            update_rest(*unit_of(t), t - whole)
        if waiting and (waiting[0] < t):
            finish_next()
    while waiting:
        finish_next()

    for p in range(2):
        ended = pl.ds(0, (bulk + 1 - p) // 2 * SLAB)
        for k in range(1, n):
            row_copy(p, k, me, ended).wait_send()
            row_copy(p, k, lax.rem(me + n - k, n), ended).wait_recv()


def store_kernel(n, pieces, bulk, gate, up, ready, out_g, out_u, sem, ready_sem):
    height = gate.shape[0] // pieces
    rows = gate.shape[0] // n
    mine = pl.ds(pl.multiple_of(lax.axis_index("rows") * rows, rows), rows)
    ends = ((bulk + 1) // 2 * SLAB, bulk // 2 * SLAB)
    outs = (out_g, out_u)
    copies = []
    for p, source in enumerate((gate, up)):
        for i in range(pieces):
            at = (pl.ds(i * height, height), pl.ds(0, ends[p]))
            pltpu.make_async_copy(source.at[at], outs[p].at[at], sem.at[p]).start()
        at = (slice(None), pl.ds(0, ends[p]))
        copies.append(pltpu.make_async_copy(source.at[at], outs[p].at[at], sem.at[p]))
    for u in range(READY):
        j, p = unit_of(bulk + u)
        copies.append(
            pltpu.make_async_copy(ready.at[u], outs[p].at[mine, pl.ds(j * SLAB, SLAB)], ready_sem.at[u])
        )
        copies[-1].start()
    for copy in copies:
        copy.wait()


def rest_kernel(n, bulk, *refs):
    peers_ready, own, peers = refs[: n - 1], refs[n - 1], refs[n : 2 * n - 1]
    col_g, col_u, _, _, out_g, out_u, out_cg, out_cu, block, last, sem, ready_sem, col_sem, last_sem = refs[2 * n - 1 :]
    rows = own.shape[1] - 8
    chunk = min(rows, 256)
    whole = bulk + READY
    me = lax.axis_index("rows")
    outs, cols, out_cols = (out_g, out_u), (col_g, col_u), (out_cg, out_cu)
    copies = []

    def begin(source, target, semaphore):
        copies.append(pltpu.make_async_copy(source, target, semaphore))
        copies[-1].start()

    def place(k):
        return pl.ds(pl.multiple_of(lax.rem(me + n - k, n) * rows, rows), rows)

    for u in range(READY):
        j, p = unit_of(bulk + u)
        for k, peer in enumerate(peers_ready, 1):
            begin(peer.at[u], outs[p].at[place(k), pl.ds(j * SLAB, SLAB)], ready_sem.at[u, k - 1])
    for p in range(2):
        at = (slice(None), pl.ds(0, (whole + 1 - p) // 2 * SLAB))
        begin(cols[p].at[at], out_cols[p].at[at], col_sem.at[p])
    for u in range(REST):
        j, p = unit_of(whole + u)
        at_columns = pl.ds(j * SLAB, SLAB)
        total = own[u, pl.ds(rows, 8), :]
        for peer in peers:
            total = total + peer[u, pl.ds(rows, 8), :]
        mean = jnp.sum(total, axis=0, keepdims=True) / (n * rows)
        last[u] = mean
        begin(last.at[u], out_cols[p].at[:, at_columns], last_sem.at[u])
        factor = 1.0 / mean
        for k, source in enumerate((own, *peers)):
            owner = lax.rem(me + n - k, n)

            def body(c, carry):
                at = pl.ds(pl.multiple_of(c * chunk, chunk), chunk)
                to = pl.ds(pl.multiple_of(owner * rows + c * chunk, chunk), chunk)
                block[u, to, :] = (source[u, at, :] * factor).astype(jnp.bfloat16)
                return carry

            lax.fori_loop(0, rows // chunk, body, 0)
            begin(block.at[u, place(k)], outs[p].at[place(k), at_columns], sem.at[u, k])
    for copy in copies:
        copy.wait()


def solution(mesh):
    n = mesh.shape["rows"]

    def shards(weight_gate, moment_gate, square_gate, weight_up, moment_up, square_up, norm_gain):
        rows, width = weight_gate.shape
        units = 2 * (width // SLAB)
        bulk = units - REST - READY
        peers = max(n - 1, 1)
        any_space = pl.BlockSpec(memory_space=pl.ANY)
        in_vmem = pl.BlockSpec(memory_space=pltpu.VMEM)
        full = ((n * rows, width), jnp.bfloat16)
        column = ((1, width), jnp.float32)
        dma = pltpu.SemaphoreType.DMA
        gate, up, col_g, col_u, ready, rest = pl.pallas_call(
            functools.partial(exchange_kernel, n),
            out_shape=tuple(
                pltpu.VMEM(*shape)
                for shape in (
                    full, full, column, column,
                    ((READY, rows, SLAB), jnp.bfloat16), ((REST, rows + 8, SLAB), jnp.float32),
                )
            ),
            in_specs=[any_space] * 6 + [pl.BlockSpec(memory_space=pltpu.HBM)],
            out_specs=[in_vmem] * 6,
            scratch_shapes=[
                pltpu.VMEM((SLOTS, 3, rows, SLAB), jnp.float32),
                pltpu.VMEM((2, rows, SLAB), jnp.float32),
                pltpu.VMEM((rows // LANES, LANES), jnp.float32),
                pltpu.VMEM((rows, LANES), jnp.float32),
                pltpu.VMEM((rows, LANES), jnp.float32),
                pltpu.VMEM((units, n, 8, SLAB), jnp.float32),
                dma((SLOTS,)),
                dma((RING, peers)),
                dma((RING, peers)),
                dma((2, peers)),
                dma((2, peers)),
                dma,
                dma((rows // min(rows, 256),)),
            ],
            compiler_params=pltpu.CompilerParams(
                collective_id=0, has_side_effects=True, vmem_limit_bytes=36 * 1024 * 1024
            ),
            name="exchange",
        )(
            weight_gate, moment_gate, square_gate, weight_up, moment_up, square_up,
            norm_gain.reshape(rows // LANES, LANES),
        )

        def from_peers(own):
            return [lax.ppermute(own, "rows", [(i, (i + k) % n) for i in range(n)]) for k in range(1, n)]

        others = from_peers(rest)
        others_ready = from_peers(ready)
        pieces = 4
        out_g, out_u = pl.pallas_call(
            functools.partial(store_kernel, n, pieces, bulk),
            out_shape=(jax.ShapeDtypeStruct(*full),) * 2,
            in_specs=[in_vmem] * 3,
            out_specs=[any_space] * 2,
            scratch_shapes=[dma((2,)), dma((READY,))],
            compiler_params=pltpu.CompilerParams(vmem_limit_bytes=1024 * 1024),
            cost_estimate=pl.CostEstimate(flops=200_000_000, bytes_accessed=4 * n * rows * width, transcendentals=0),
            name="store",
        )(gate, up, ready)
        first = 2 * n + 1
        out_g, out_u, out_cg, out_cu = pl.pallas_call(
            functools.partial(rest_kernel, n, bulk),
            out_shape=(jax.ShapeDtypeStruct(*full),) * 2 + (jax.ShapeDtypeStruct(*column),) * 2,
            in_specs=[in_vmem] * first + [any_space] * 2,
            out_specs=[any_space] * 4,
            input_output_aliases={first: 0, first + 1: 1},
            scratch_shapes=[
                pltpu.VMEM((REST, n * rows, SLAB), jnp.bfloat16),
                pltpu.VMEM((REST, 1, SLAB), jnp.float32),
                dma((REST, n)),
                dma((READY, peers)),
                dma((2,)),
                dma((REST,)),
            ],
            compiler_params=pltpu.CompilerParams(vmem_limit_bytes=8 * 1024 * 1024),
            name="rest",
        )(*others_ready, rest, *others, col_g, col_u, out_g, out_u)
        return out_g, out_u, out_cg.reshape(width), out_cu.reshape(width)

    held = P(("trial", "rows"), "cols")
    return jax.shard_map(
        shards,
        mesh=mesh,
        in_specs=(held,) * 6 + (P(("trial", "rows")),),
        out_specs=(P("trial", "cols"), P("trial", "cols"), P(("trial", "cols")), P(("trial", "cols"))),
        check_vma=False,
    )
```

```python
import functools

import jax
import jax.numpy as jnp
from jax import lax
from jax.experimental import pallas as pl
from jax.experimental.pallas import tpu as pltpu
from jax.sharding import PartitionSpec as P

learn_rate = 0.02
decay_rate = 0.05
tiny_value = 1e-08

LANES = 128
SLAB = 256
SLOTS = 4
RING = 4
READY = 1
REST = 2
MESH = pl.DeviceIdType.MESH


def unit_of(t):
    return t // 2, t % 2


def halves(value):
    high = value.astype(jnp.bfloat16)
    return high, (value - high.astype(jnp.float32)).astype(jnp.bfloat16)


def exchange_kernel(
    n, wg, mg, sg, wu, mu, su, gain_hbm, out_g, out_u, col_g, col_u, parcel,
    buf, held, gain, keep_scale, step_scale, parts,
    in_sem, part_send, part_recv, row_send, row_recv, piece_sem,
):
    rows, width = wg.shape
    units = 2 * (width // SLAB)
    whole = units - REST
    bulk = whole - READY
    chunk = min(rows, 256)
    me = lax.axis_index("rows")
    sources = ((wg, mg, sg), (wu, mu, su))
    outs = (out_g, out_u)
    cols = (col_g, col_u)

    def columns(j):
        return pl.ds(pl.multiple_of(j * SLAB, SLAB), SLAB)

    def loads(j, p):
        slot = lax.rem(2 * j + p, SLOTS)
        return [
            pltpu.make_async_copy(source.at[:, columns(j)], buf.at[slot, i], in_sem.at[slot])
            for i, source in enumerate(sources[p])
        ]

    def loaded(slot):
        pltpu.make_async_copy(buf.at[slot], buf.at[slot], in_sem.at[slot]).wait()

    def piece_loads(c):
        j, p = unit_of(units - 1)
        at = pl.ds(pl.multiple_of(c * chunk, chunk), chunk)
        return [
            pltpu.make_async_copy(source.at[at, columns(j)], buf.at[(units - 1) % SLOTS, i, at], piece_sem.at[c])
            for i, source in enumerate(sources[p])
        ]

    def piece_loaded(c):
        block = buf.at[(units - 1) % SLOTS, :, pl.ds(pl.multiple_of(c * chunk, chunk), chunk)]
        pltpu.make_async_copy(block, block, piece_sem.at[c]).wait()

    def part_copy(j, p, k, owner):
        t = 2 * j + p
        return pltpu.make_async_remote_copy(
            src_ref=parts.at[t, owner],
            dst_ref=parts.at[t, owner],
            send_sem=part_send.at[lax.rem(t, 2), k - 1],
            recv_sem=part_recv.at[lax.rem(t, RING), k - 1],
            device_id={"rows": lax.rem(me + k, n)},
            device_id_type=MESH,
        )

    def row_copy(p, k, owner, at_columns):
        block = outs[p].at[pl.ds(pl.multiple_of(owner * rows, rows), rows), at_columns]
        return pltpu.make_async_remote_copy(
            src_ref=block,
            dst_ref=block,
            send_sem=row_send.at[p, k - 1],
            recv_sem=row_recv.at[p, k - 1],
            device_id={"rows": lax.rem(me + k, n)},
            device_id_type=MESH,
        )

    zero = jnp.zeros((8, LANES), jnp.float32)

    def update(j, p, keep_value, pieces=False):
        slot = lax.rem(2 * j + p, SLOTS)
        if not pieces:
            loaded(slot)

        def body(c, sums):
            if pieces:
                piece_loaded(c)
            at = pl.ds(pl.multiple_of(c * chunk, chunk), chunk)
            keep, scale = keep_scale[at, :], step_scale[at, :]
            new = []
            for i in range(SLAB // LANES):
                tile = pl.ds(i * LANES, LANES)
                square = buf[slot, 2, at, tile]
                root = square * lax.rsqrt(square)
                value = buf[slot, 0, at, tile] * keep - (buf[slot, 1, at, tile] * scale) / (root + tiny_value)
                keep_value(at, tile, value)
                new.append(sums[i] + jnp.sum(jnp.abs(value).reshape(chunk // 8, 8, LANES), axis=0))
            return tuple(new)

        return lax.fori_loop(0, rows // chunk, body, (zero,) * (SLAB // LANES))

    def update_shared(j, p):
        def keep_value(at, tile, value):
            held[p, at, tile] = value

        sums = update(j, p, keep_value)
        for i in range(SLAB // LANES):
            parts[2 * j + p, me, :, pl.ds(i * LANES, LANES)] = sums[i]
        for k in range(1, n):
            part_copy(j, p, k, me).start()

    def update_rest(j, p, u):
        high, low = READY + 2 * u, READY + 2 * u + 1

        def keep_value(at, tile, value):
            parcel[high, at, tile], parcel[low, at, tile] = halves(value)

        sums = update(j, p, keep_value, pieces=2 * j + p == units - 1)
        tail = pl.ds(rows, 16)
        for i in range(SLAB // LANES):
            lanes = pl.ds(i * LANES, LANES)
            first, second = halves(sums[i])
            third = sums[i] - first.astype(jnp.float32) - second.astype(jnp.float32)
            parcel[high, tail, lanes] = jnp.concatenate([first.astype(jnp.float32), second.astype(jnp.float32)]).astype(jnp.bfloat16)
            parcel[low, tail, lanes] = jnp.concatenate([third, zero]).astype(jnp.bfloat16)

    def factor_of(j, p):
        t = 2 * j + p
        for k in range(1, n):
            part_copy(j, p, k, lax.rem(me + n - k, n)).wait_recv()
            part_copy(j, p, k, me).wait_send()
        total = parts[t, 0]
        for r in range(1, n):
            total = total + parts[t, r]
        column = jnp.sum(total, axis=0, keepdims=True) / (n * rows)
        cols[p][:, columns(j)] = column
        return 1.0 / column

    def finish_ready(j, p):
        factor = factor_of(j, p)

        def body(c, carry):
            at = pl.ds(pl.multiple_of(c * chunk, chunk), chunk)
            parcel[2 * j + p - bulk, at, :] = (held[p, at, :] * factor).astype(jnp.bfloat16)
            return carry

        lax.fori_loop(0, rows // chunk, body, 0)

    def finish(j, p):
        factor = factor_of(j, p)

        def body(c, carry):
            at = pl.ds(pl.multiple_of(c * chunk, chunk), chunk)
            to = pl.ds(pl.multiple_of(me * rows + c * chunk, chunk), chunk)
            outs[p][to, columns(j)] = (held[p, at, :] * factor).astype(jnp.bfloat16)
            return carry

        lax.fori_loop(0, rows // chunk, body, 0)
        for k in range(1, n):
            row_copy(p, k, me, columns(j)).start()

    gain_copy = pltpu.make_async_copy(gain_hbm, gain, piece_sem.at[0])
    gain_copy.start()
    ahead = min(SLOTS, units)

    def begin(j, carry):
        for p in range(2):
            for copy in loads(j, p):
                copy.start()
        return carry

    lax.fori_loop(0, ahead // 2, begin, 0)

    barrier = pltpu.get_barrier_semaphore()
    for k in range(1, n):
        pl.semaphore_signal(barrier, inc=1, device_id={"rows": lax.rem(me + k, n)}, device_id_type=MESH)

    gain_copy.wait()
    for r in range(rows // LANES):
        spread = jnp.broadcast_to(gain[r : r + 1, :], (LANES, LANES)).T
        at = pl.ds(r * LANES, LANES)
        keep_scale[at, :] = spread * (1.0 - learn_rate * decay_rate)
        step_scale[at, :] = spread * learn_rate

    pl.semaphore_wait(barrier, n - 1)

    def refill(j, p):
        @pl.when(2 * j + p + ahead < units - 1)
        def _():
            for copy in loads(j + ahead // 2, p):
                copy.start()

        if p == (units - 1) % 2:

            @pl.when(2 * j + p + ahead == units - 1)
            def _():
                for c in range(rows // chunk):
                    for copy in piece_loads(c):
                        copy.start()

    def step(j, carry):
        update_shared(j, 0)
        refill(j, 0)

        @pl.when(j > 0)
        def _():
            finish(j - 1, 1)

        update_shared(j, 1)
        refill(j, 1)
        finish(j, 0)
        return carry

    lax.fori_loop(0, bulk // 2, step, 0)
    waiting = [bulk // 2 * 2 - 1]

    def finish_next():
        t = waiting.pop(0)
        (finish if t < bulk else finish_ready)(*unit_of(t))

    for t in range(bulk // 2 * 2, units):
        if t < whole:
            update_shared(*unit_of(t))
            waiting.append(t)
        else:
            update_rest(*unit_of(t), t - whole)
        if waiting and (waiting[0] < t):
            finish_next()
    while waiting:
        finish_next()

    for p in range(2):
        ended = pl.ds(0, (bulk + 1 - p) // 2 * SLAB)
        for k in range(1, n):
            row_copy(p, k, me, ended).wait_send()
            row_copy(p, k, lax.rem(me + n - k, n), ended).wait_recv()


def store_kernel(n, pieces, bulk, gate, up, parcel, out_g, out_u, sem, ready_sem):
    height = gate.shape[0] // pieces
    rows = gate.shape[0] // n
    mine = pl.ds(pl.multiple_of(lax.axis_index("rows") * rows, rows), rows)
    ends = ((bulk + 1) // 2 * SLAB, bulk // 2 * SLAB)
    outs = (out_g, out_u)
    copies = []
    for p, source in enumerate((gate, up)):
        for i in range(pieces):
            at = (pl.ds(i * height, height), pl.ds(0, ends[p]))
            pltpu.make_async_copy(source.at[at], outs[p].at[at], sem.at[p]).start()
        at = (slice(None), pl.ds(0, ends[p]))
        copies.append(pltpu.make_async_copy(source.at[at], outs[p].at[at], sem.at[p]))
    for u in range(READY):
        j, p = unit_of(bulk + u)
        copies.append(
            pltpu.make_async_copy(parcel.at[u, pl.ds(0, rows)], outs[p].at[mine, pl.ds(j * SLAB, SLAB)], ready_sem.at[u])
        )
        copies[-1].start()
    for copy in copies:
        copy.wait()


def rest_kernel(n, bulk, *refs):
    own, peers = refs[0], refs[1:n]
    col_g, col_u, _, _, out_g, out_u, out_cg, out_cu, block, last, sem, ready_sem, col_sem = refs[n:]
    rows = own.shape[1] - 16
    chunk = min(rows, 256)
    whole = bulk + READY
    me = lax.axis_index("rows")
    outs, cols, out_cols = (out_g, out_u), (col_g, col_u), (out_cg, out_cu)
    def begin(source, target, semaphore):
        pltpu.make_async_copy(source, target, semaphore).start()

    def end(target, semaphore):
        pltpu.make_async_copy(target, target, semaphore).wait()

    def place(k):
        return pl.ds(pl.multiple_of(lax.rem(me + n - k, n) * rows, rows), rows)

    for u in range(READY):
        j, p = unit_of(bulk + u)
        for k, peer in enumerate(peers, 1):
            begin(peer.at[u, pl.ds(0, rows)], outs[p].at[place(k), pl.ds(j * SLAB, SLAB)], ready_sem.at[u])
    for p in range(2):
        at = (slice(None), pl.ds(0, (whole + 1 - p) // 2 * SLAB))
        begin(cols[p].at[at], out_cols[p].at[at], col_sem.at[p])
    for u in range(REST):
        j, p = unit_of(whole + u)
        at_columns = pl.ds(j * SLAB, SLAB)
        high, low = READY + 2 * u, READY + 2 * u + 1
        total = jnp.zeros((8, SLAB), jnp.float32)
        for source in (own, *peers):
            upper = source[high, pl.ds(rows, 16), :].astype(jnp.float32)
            lower = source[low, pl.ds(rows, 16), :].astype(jnp.float32)
            total = total + (upper[:8] + upper[8:] + lower[:8])
        mean = jnp.sum(total, axis=0, keepdims=True) / (n * rows)
        last[u] = mean
        begin(last.at[u], out_cols[p].at[:, at_columns], col_sem.at[p])
        factor = 1.0 / mean
        for k, source in enumerate((own, *peers)):
            owner = lax.rem(me + n - k, n)

            def body(c, carry):
                at = pl.ds(pl.multiple_of(c * chunk, chunk), chunk)
                to = pl.ds(pl.multiple_of(owner * rows + c * chunk, chunk), chunk)
                value = source[high, at, :].astype(jnp.float32) + source[low, at, :].astype(jnp.float32)
                block[u, to, :] = (value * factor).astype(jnp.bfloat16)
                return carry

            lax.fori_loop(0, rows // chunk, body, 0)
            begin(block.at[u, place(k)], outs[p].at[place(k), at_columns], sem.at[u])
    for u in range(READY):
        j, p = unit_of(bulk + u)
        if n > 1:
            end(outs[p].at[pl.ds(0, (n - 1) * rows), pl.ds(j * SLAB, SLAB)], ready_sem.at[u])
    for u in range(REST):
        j, p = unit_of(whole + u)
        end(outs[p].at[:, pl.ds(j * SLAB, SLAB)], sem.at[u])
    for p in range(2):
        end(out_cols[p], col_sem.at[p])


def solution(mesh):
    n = mesh.shape["rows"]

    def shards(weight_gate, moment_gate, square_gate, weight_up, moment_up, square_up, norm_gain):
        rows, width = weight_gate.shape
        units = 2 * (width // SLAB)
        bulk = units - REST - READY
        peers = max(n - 1, 1)
        any_space = pl.BlockSpec(memory_space=pl.ANY)
        in_vmem = pl.BlockSpec(memory_space=pltpu.VMEM)
        full = ((n * rows, width), jnp.bfloat16)
        column = ((1, width), jnp.float32)
        dma = pltpu.SemaphoreType.DMA
        gate, up, col_g, col_u, parcel = pl.pallas_call(
            functools.partial(exchange_kernel, n),
            out_shape=tuple(
                pltpu.VMEM(*shape)
                for shape in (
                    full, full, column, column,
                    ((READY + 2 * REST, rows + 16, SLAB), jnp.bfloat16),
                )
            ),
            in_specs=[any_space] * 6 + [pl.BlockSpec(memory_space=pltpu.HBM)],
            out_specs=[in_vmem] * 5,
            scratch_shapes=[
                pltpu.VMEM((SLOTS, 3, rows, SLAB), jnp.float32),
                pltpu.VMEM((2, rows, SLAB), jnp.float32),
                pltpu.VMEM((rows // LANES, LANES), jnp.float32),
                pltpu.VMEM((rows, LANES), jnp.float32),
                pltpu.VMEM((rows, LANES), jnp.float32),
                pltpu.VMEM((units, n, 8, SLAB), jnp.float32),
                dma((SLOTS,)),
                dma((2, peers)),
                dma((RING, peers)),
                dma((2, peers)),
                dma((2, peers)),
                dma((rows // min(rows, 256),)),
            ],
            compiler_params=pltpu.CompilerParams(
                collective_id=0, has_side_effects=True, vmem_limit_bytes=36 * 1024 * 1024
            ),
            name="exchange",
        )(
            weight_gate, moment_gate, square_gate, weight_up, moment_up, square_up,
            norm_gain.reshape(rows // LANES, LANES),
        )

        others = [
            lax.ppermute(parcel, "rows", [(i, (i + k) % n) for i in range(n)]) for k in range(1, n)
        ]
        pieces = 4
        out_g, out_u = pl.pallas_call(
            functools.partial(store_kernel, n, pieces, bulk),
            out_shape=(jax.ShapeDtypeStruct(*full),) * 2,
            in_specs=[in_vmem] * 3,
            out_specs=[any_space] * 2,
            scratch_shapes=[dma((2,)), dma((READY,))],
            compiler_params=pltpu.CompilerParams(vmem_limit_bytes=1024 * 1024),
            cost_estimate=pl.CostEstimate(flops=200_000_000, bytes_accessed=4 * n * rows * width, transcendentals=0),
            name="store",
        )(gate, up, parcel)
        first = n + 2
        out_g, out_u, out_cg, out_cu = pl.pallas_call(
            functools.partial(rest_kernel, n, bulk),
            out_shape=(jax.ShapeDtypeStruct(*full),) * 2 + (jax.ShapeDtypeStruct(*column),) * 2,
            in_specs=[in_vmem] * first + [any_space] * 2,
            out_specs=[any_space] * 4,
            input_output_aliases={first: 0, first + 1: 1},
            scratch_shapes=[
                pltpu.VMEM((REST, n * rows, SLAB), jnp.bfloat16),
                pltpu.VMEM((REST, 1, SLAB), jnp.float32),
                dma((REST,)),
                dma((READY,)),
                dma((2,)),
            ],
            compiler_params=pltpu.CompilerParams(vmem_limit_bytes=8 * 1024 * 1024),
            name="rest",
        )(parcel, *others, col_g, col_u, out_g, out_u)
        return out_g, out_u, out_cg.reshape(width), out_cu.reshape(width)

    held = P(("trial", "rows"), "cols")
    return jax.shard_map(
        shards,
        mesh=mesh,
        in_specs=(held,) * 6 + (P(("trial", "rows")),),
        out_specs=(P("trial", "cols"), P("trial", "cols"), P(("trial", "cols")), P(("trial", "cols"))),
        check_vma=False,
    )
```

```python
import functools

import jax
import jax.numpy as jnp
from jax import lax
from jax.experimental import pallas as pl
from jax.experimental.pallas import tpu as pltpu
from jax.sharding import PartitionSpec as P

learn_rate = 0.02
decay_rate = 0.05
tiny_value = 1e-08

LANES = 128
SLAB = 256
SLOTS = 4
RING = 4
READY = 1
REST = 2
MESH = pl.DeviceIdType.MESH


def unit_of(t):
    return t // 2, t % 2


def halves(value):
    high = value.astype(jnp.bfloat16)
    return high, (value - high.astype(jnp.float32)).astype(jnp.bfloat16)


def exchange_kernel(
    n, wg, mg, sg, wu, mu, su, gain_hbm, out_g, out_u, col_g, col_u, parcel,
    buf, held, gain, keep_scale, step_scale, parts,
    in_sem, part_send, part_recv, row_send, row_recv, piece_sem,
):
    rows, width = wg.shape
    units = 2 * (width // SLAB)
    whole = units - REST
    bulk = whole - READY
    chunk = min(rows, 256)
    me = lax.axis_index("rows")
    sources = ((wg, mg, sg), (wu, mu, su))
    outs = (out_g, out_u)
    cols = (col_g, col_u)

    def columns(j):
        return pl.ds(pl.multiple_of(j * SLAB, SLAB), SLAB)

    def loads(j, p):
        slot = lax.rem(2 * j + p, SLOTS)
        return [
            pltpu.make_async_copy(source.at[:, columns(j)], buf.at[slot, i], in_sem.at[slot])
            for i, source in enumerate(sources[p])
        ]

    def loaded(slot):
        pltpu.make_async_copy(buf.at[slot], buf.at[slot], in_sem.at[slot]).wait()

    def piece_loads(c):
        j, p = unit_of(units - 1)
        at = pl.ds(pl.multiple_of(c * chunk, chunk), chunk)
        return [
            pltpu.make_async_copy(source.at[at, columns(j)], buf.at[(units - 1) % SLOTS, i, at], piece_sem.at[c])
            for i, source in enumerate(sources[p])
        ]

    def piece_loaded(c):
        block = buf.at[(units - 1) % SLOTS, :, pl.ds(pl.multiple_of(c * chunk, chunk), chunk)]
        pltpu.make_async_copy(block, block, piece_sem.at[c]).wait()

    def part_copy(j, p, k, owner):
        t = 2 * j + p
        return pltpu.make_async_remote_copy(
            src_ref=parts.at[t, owner],
            dst_ref=parts.at[t, owner],
            send_sem=part_send.at[lax.rem(t, 2), k - 1],
            recv_sem=part_recv.at[lax.rem(t, RING), k - 1],
            device_id={"rows": lax.rem(me + k, n)},
            device_id_type=MESH,
        )

    def row_copy(p, k, owner, at_columns, c=0, height=None):
        height = height or rows
        block = outs[p].at[pl.ds(pl.multiple_of(owner * rows + c * height, height), height), at_columns]
        return pltpu.make_async_remote_copy(
            src_ref=block,
            dst_ref=block,
            send_sem=row_send.at[p, k - 1],
            recv_sem=row_recv.at[p, k - 1],
            device_id={"rows": lax.rem(me + k, n)},
            device_id_type=MESH,
        )

    zero = jnp.zeros((8, LANES), jnp.float32)

    def update(j, p, keep_value, pieces=False):
        slot = lax.rem(2 * j + p, SLOTS)
        if not pieces:
            loaded(slot)

        def body(c, sums):
            if pieces:
                piece_loaded(c)
            at = pl.ds(pl.multiple_of(c * chunk, chunk), chunk)
            keep, scale = keep_scale[at, :], step_scale[at, :]
            new = []
            for i in range(SLAB // LANES):
                tile = pl.ds(i * LANES, LANES)
                square = buf[slot, 2, at, tile]
                root = square * lax.rsqrt(square)
                value = buf[slot, 0, at, tile] * keep - (buf[slot, 1, at, tile] * scale) / (root + tiny_value)
                keep_value(at, tile, value)
                new.append(sums[i] + jnp.sum(jnp.abs(value).reshape(chunk // 8, 8, LANES), axis=0))
            return tuple(new)

        return lax.fori_loop(0, rows // chunk, body, (zero,) * (SLAB // LANES))

    def update_shared(j, p):
        def keep_value(at, tile, value):
            held[p, at, tile] = value

        sums = update(j, p, keep_value)
        for i in range(SLAB // LANES):
            parts[2 * j + p, me, :, pl.ds(i * LANES, LANES)] = sums[i]
        for k in range(1, n):
            part_copy(j, p, k, me).start()

    def update_rest(j, p, u):
        high, low = READY + 2 * u, READY + 2 * u + 1

        def keep_value(at, tile, value):
            parcel[high, at, tile], parcel[low, at, tile] = halves(value)

        sums = update(j, p, keep_value, pieces=2 * j + p == units - 1)
        tail = pl.ds(rows, 16)
        for i in range(SLAB // LANES):
            lanes = pl.ds(i * LANES, LANES)
            first, second = halves(sums[i])
            third = sums[i] - first.astype(jnp.float32) - second.astype(jnp.float32)
            parcel[high, tail, lanes] = jnp.concatenate([first.astype(jnp.float32), second.astype(jnp.float32)]).astype(jnp.bfloat16)
            parcel[low, tail, lanes] = jnp.concatenate([third, zero]).astype(jnp.bfloat16)

    def factor_of(j, p):
        t = 2 * j + p
        for k in range(1, n):
            part_copy(j, p, k, lax.rem(me + n - k, n)).wait_recv()
            part_copy(j, p, k, me).wait_send()
        total = parts[t, 0]
        for r in range(1, n):
            total = total + parts[t, r]
        column = jnp.sum(total, axis=0, keepdims=True) / (n * rows)
        cols[p][:, columns(j)] = column
        return 1.0 / column

    def finish_ready(j, p):
        factor = factor_of(j, p)

        def body(c, carry):
            at = pl.ds(pl.multiple_of(c * chunk, chunk), chunk)
            parcel[2 * j + p - bulk, at, :] = (held[p, at, :] * factor).astype(jnp.bfloat16)
            return carry

        lax.fori_loop(0, rows // chunk, body, 0)

    def finish(j, p):
        factor = factor_of(j, p)

        def body(c, carry):
            at = pl.ds(pl.multiple_of(c * chunk, chunk), chunk)
            to = pl.ds(pl.multiple_of(me * rows + c * chunk, chunk), chunk)
            outs[p][to, columns(j)] = (held[p, at, :] * factor).astype(jnp.bfloat16)
            for k in range(1, n):
                row_copy(p, k, me, columns(j), c, chunk).start()
            return carry

        lax.fori_loop(0, rows // chunk, body, 0)

    gain_copy = pltpu.make_async_copy(gain_hbm, gain, piece_sem.at[0])
    gain_copy.start()
    ahead = min(SLOTS, units)

    def begin(j, carry):
        for p in range(2):
            for copy in loads(j, p):
                copy.start()
        return carry

    lax.fori_loop(0, ahead // 2, begin, 0)

    barrier = pltpu.get_barrier_semaphore()
    for k in range(1, n):
        pl.semaphore_signal(barrier, inc=1, device_id={"rows": lax.rem(me + k, n)}, device_id_type=MESH)

    gain_copy.wait()
    for r in range(rows // LANES):
        spread = jnp.broadcast_to(gain[r : r + 1, :], (LANES, LANES)).T
        at = pl.ds(r * LANES, LANES)
        keep_scale[at, :] = spread * (1.0 - learn_rate * decay_rate)
        step_scale[at, :] = spread * learn_rate

    pl.semaphore_wait(barrier, n - 1)

    def refill(j, p):
        @pl.when(2 * j + p + ahead < units - 1)
        def _():
            for copy in loads(j + ahead // 2, p):
                copy.start()

        if p == (units - 1) % 2:

            @pl.when(2 * j + p + ahead == units - 1)
            def _():
                for c in range(rows // chunk):
                    for copy in piece_loads(c):
                        copy.start()

    def step(j, carry):
        update_shared(j, 0)
        refill(j, 0)

        @pl.when(j > 0)
        def _():
            finish(j - 1, 1)

        update_shared(j, 1)
        refill(j, 1)
        finish(j, 0)
        return carry

    lax.fori_loop(0, bulk // 2, step, 0)
    waiting = [bulk // 2 * 2 - 1]

    def finish_next():
        t = waiting.pop(0)
        (finish if t < bulk else finish_ready)(*unit_of(t))

    for t in range(bulk // 2 * 2, units):
        if t < whole:
            update_shared(*unit_of(t))
            waiting.append(t)
        else:
            update_rest(*unit_of(t), t - whole)
        if waiting and (waiting[0] < t):
            finish_next()
    while waiting:
        finish_next()

    for p in range(2):
        ended = pl.ds(0, (bulk + 1 - p) // 2 * SLAB)
        for k in range(1, n):
            row_copy(p, k, me, ended).wait_send()
            row_copy(p, k, lax.rem(me + n - k, n), ended).wait_recv()


def store_kernel(n, pieces, bulk, gate, up, parcel, out_g, out_u, sem, ready_sem):
    height = gate.shape[0] // pieces
    rows = gate.shape[0] // n
    mine = pl.ds(pl.multiple_of(lax.axis_index("rows") * rows, rows), rows)
    ends = ((bulk + 1) // 2 * SLAB, bulk // 2 * SLAB)
    outs = (out_g, out_u)
    copies = []
    for p, source in enumerate((gate, up)):
        for i in range(pieces):
            at = (pl.ds(i * height, height), pl.ds(0, ends[p]))
            pltpu.make_async_copy(source.at[at], outs[p].at[at], sem.at[p]).start()
        at = (slice(None), pl.ds(0, ends[p]))
        copies.append(pltpu.make_async_copy(source.at[at], outs[p].at[at], sem.at[p]))
    for u in range(READY):
        j, p = unit_of(bulk + u)
        copies.append(
            pltpu.make_async_copy(parcel.at[u, pl.ds(0, rows)], outs[p].at[mine, pl.ds(j * SLAB, SLAB)], ready_sem.at[u])
        )
        copies[-1].start()
    for copy in copies:
        copy.wait()


def rest_kernel(n, bulk, *refs):
    own, peers = refs[0], refs[1:n]
    col_g, col_u, _, _, out_g, out_u, out_cg, out_cu, block, last, sem, ready_sem, col_sem = refs[n:]
    rows = own.shape[1] - 16
    chunk = min(rows, 256)
    whole = bulk + READY
    me = lax.axis_index("rows")
    outs, cols, out_cols = (out_g, out_u), (col_g, col_u), (out_cg, out_cu)
    def begin(source, target, semaphore):
        pltpu.make_async_copy(source, target, semaphore).start()

    def end(target, semaphore):
        pltpu.make_async_copy(target, target, semaphore).wait()

    def place(k):
        return pl.ds(pl.multiple_of(lax.rem(me + n - k, n) * rows, rows), rows)

    for u in range(READY):
        j, p = unit_of(bulk + u)
        for k, peer in enumerate(peers, 1):
            begin(peer.at[u, pl.ds(0, rows)], outs[p].at[place(k), pl.ds(j * SLAB, SLAB)], ready_sem.at[u])
    for p in range(2):
        at = (slice(None), pl.ds(0, (whole + 1 - p) // 2 * SLAB))
        begin(cols[p].at[at], out_cols[p].at[at], col_sem.at[p])
    for u in range(REST):
        j, p = unit_of(whole + u)
        at_columns = pl.ds(j * SLAB, SLAB)
        high, low = READY + 2 * u, READY + 2 * u + 1
        total = jnp.zeros((8, SLAB), jnp.float32)
        for source in (own, *peers):
            upper = source[high, pl.ds(rows, 16), :].astype(jnp.float32)
            lower = source[low, pl.ds(rows, 16), :].astype(jnp.float32)
            total = total + (upper[:8] + upper[8:] + lower[:8])
        mean = jnp.sum(total, axis=0, keepdims=True) / (n * rows)
        last[u] = mean
        begin(last.at[u], out_cols[p].at[:, at_columns], col_sem.at[p])
        factor = 1.0 / mean
        for k, source in enumerate((own, *peers)):
            owner = lax.rem(me + n - k, n)

            def body(c, carry):
                at = pl.ds(pl.multiple_of(c * chunk, chunk), chunk)
                to = pl.ds(pl.multiple_of(owner * rows + c * chunk, chunk), chunk)
                value = source[high, at, :].astype(jnp.float32) + source[low, at, :].astype(jnp.float32)
                block[u, to, :] = (value * factor).astype(jnp.bfloat16)
                return carry

            lax.fori_loop(0, rows // chunk, body, 0)
            begin(block.at[u, place(k)], outs[p].at[place(k), at_columns], sem.at[u])
    for u in range(READY):
        j, p = unit_of(bulk + u)
        if n > 1:
            end(outs[p].at[pl.ds(0, (n - 1) * rows), pl.ds(j * SLAB, SLAB)], ready_sem.at[u])
    for u in range(REST):
        j, p = unit_of(whole + u)
        end(outs[p].at[:, pl.ds(j * SLAB, SLAB)], sem.at[u])
    for p in range(2):
        end(out_cols[p], col_sem.at[p])


def solution(mesh):
    n = mesh.shape["rows"]

    def shards(weight_gate, moment_gate, square_gate, weight_up, moment_up, square_up, norm_gain):
        rows, width = weight_gate.shape
        units = 2 * (width // SLAB)
        bulk = units - REST - READY
        peers = max(n - 1, 1)
        any_space = pl.BlockSpec(memory_space=pl.ANY)
        in_vmem = pl.BlockSpec(memory_space=pltpu.VMEM)
        full = ((n * rows, width), jnp.bfloat16)
        column = ((1, width), jnp.float32)
        dma = pltpu.SemaphoreType.DMA
        gate, up, col_g, col_u, parcel = pl.pallas_call(
            functools.partial(exchange_kernel, n),
            out_shape=tuple(
                pltpu.VMEM(*shape)
                for shape in (
                    full, full, column, column,
                    ((READY + 2 * REST, rows + 16, SLAB), jnp.bfloat16),
                )
            ),
            in_specs=[any_space] * 6 + [pl.BlockSpec(memory_space=pltpu.HBM)],
            out_specs=[in_vmem] * 5,
            scratch_shapes=[
                pltpu.VMEM((SLOTS, 3, rows, SLAB), jnp.float32),
                pltpu.VMEM((2, rows, SLAB), jnp.float32),
                pltpu.VMEM((rows // LANES, LANES), jnp.float32),
                pltpu.VMEM((rows, LANES), jnp.float32),
                pltpu.VMEM((rows, LANES), jnp.float32),
                pltpu.VMEM((units, n, 8, SLAB), jnp.float32),
                dma((SLOTS,)),
                dma((2, peers)),
                dma((RING, peers)),
                dma((2, peers)),
                dma((2, peers)),
                dma((rows // min(rows, 256),)),
            ],
            compiler_params=pltpu.CompilerParams(
                collective_id=0, has_side_effects=True, vmem_limit_bytes=36 * 1024 * 1024
            ),
            name="exchange",
        )(
            weight_gate, moment_gate, square_gate, weight_up, moment_up, square_up,
            norm_gain.reshape(rows // LANES, LANES),
        )

        others = [
            lax.ppermute(parcel, "rows", [(i, (i + k) % n) for i in range(n)]) for k in range(1, n)
        ]
        pieces = 4
        out_g, out_u = pl.pallas_call(
            functools.partial(store_kernel, n, pieces, bulk),
            out_shape=(jax.ShapeDtypeStruct(*full),) * 2,
            in_specs=[in_vmem] * 3,
            out_specs=[any_space] * 2,
            scratch_shapes=[dma((2,)), dma((READY,))],
            compiler_params=pltpu.CompilerParams(vmem_limit_bytes=1024 * 1024),
            cost_estimate=pl.CostEstimate(flops=200_000_000, bytes_accessed=4 * n * rows * width, transcendentals=0),
            name="store",
        )(gate, up, parcel)
        first = n + 2
        out_g, out_u, out_cg, out_cu = pl.pallas_call(
            functools.partial(rest_kernel, n, bulk),
            out_shape=(jax.ShapeDtypeStruct(*full),) * 2 + (jax.ShapeDtypeStruct(*column),) * 2,
            in_specs=[in_vmem] * first + [any_space] * 2,
            out_specs=[any_space] * 4,
            input_output_aliases={first: 0, first + 1: 1},
            scratch_shapes=[
                pltpu.VMEM((REST, n * rows, SLAB), jnp.bfloat16),
                pltpu.VMEM((REST, 1, SLAB), jnp.float32),
                dma((REST,)),
                dma((READY,)),
                dma((2,)),
            ],
            compiler_params=pltpu.CompilerParams(vmem_limit_bytes=8 * 1024 * 1024),
            name="rest",
        )(parcel, *others, col_g, col_u, out_g, out_u)
        return out_g, out_u, out_cg.reshape(width), out_cu.reshape(width)

    held = P(("trial", "rows"), "cols")
    return jax.shard_map(
        shards,
        mesh=mesh,
        in_specs=(held,) * 6 + (P(("trial", "rows")),),
        out_specs=(P("trial", "cols"), P("trial", "cols"), P(("trial", "cols")), P(("trial", "cols"))),
        check_vma=False,
    )
```
